128 devices in a mesh: row: 8 (over y, x_hi), col: 16 (over x_lo, z, core).
Axes of the slice: x: 4 (x_hi: 2, x_lo: 2; x = x_hi * 2 + x_lo), y: 4, z: 4, core: 2. Of those that a mesh axis runs over, the one named last changes fastest.
Arguments:
- left_matrix: float32 [4096, 4096], P('row', 'col'), may hold values from -6 to 6
- right_matrix: float32 [4096, 4096], P('row', 'col'), may hold values from -0.09375 to 0.09375
Outputs:
- product_matrix: float32 [4096, 4096], P('row', 'col')
The draws below stay inside these ranges and needn't reach their ends.
All inputs are finite; a program needn't handle non-finite values.
Results may differ from the reference program's by a relative error of at most 0.00019.
Values sent between devices are 32-bit elements; how exact they have to be, the bound alone decides.
A program may use at most 64 MiB of HBM per device.

```python
import jax
import jax.numpy as jnp
from jax import lax

ORDER = 4096


def level_of(own_key, dims, split, least, high):
    def one(position, blocks):
        steps = jax.random.uniform(jax.random.fold_in(jax.random.fold_in(own_key, 6), position), (blocks,), jnp.float32, least / len(split), high / len(split))
        return jnp.repeat(jnp.exp(steps), dims[position] // blocks).reshape((-1,) + (1,) * (len(dims) - position - 1))

    gain = one(*split[0])
    for cut in split[1:]:
        gain = gain * one(*cut)
    return gain


def scatter_about(own_key, extent, spread, reach, split=(), dtype=jnp.bfloat16):
    gain = level_of(own_key, extent, split, -0.22, 0.18) if split else 1.0
    result = jax.random.normal(own_key, extent, jnp.float32) * spread * gain
    return jnp.minimum(jnp.maximum(result, -reach), reach).astype(dtype)


def setup_inputs(seed: int = 0) -> dict:
    arg_keys = jax.random.split(jax.random.key(seed), 3)
    left_matrix = scatter_about(arg_keys[0], (ORDER, ORDER), 1.0, 6.0, ((0, 8), (1, 16)), jnp.float32)
    right_matrix = scatter_about(arg_keys[1], (ORDER, ORDER), ORDER ** -0.5, 0.09375, ((0, 8), (1, 16)), jnp.float32)
    return {"left_matrix": left_matrix, "right_matrix": right_matrix}


def multiply(left_term, right_term):
    return jnp.dot(left_term, right_term, precision=lax.Precision.HIGHEST, preferred_element_type=jnp.float32)


def left_terms(upper_left, upper_right, lower_left, lower_right):
    sum_one = lower_left + lower_right
    sum_two = sum_one - upper_left
    sum_three = upper_left - lower_left
    sum_four = upper_right - sum_two
    return (upper_left, upper_right, sum_four, lower_right, sum_one, sum_two, sum_three)


def right_terms(upper_left, upper_right, lower_left, lower_right):
    diff_one = upper_right - upper_left
    diff_two = lower_right - diff_one
    diff_three = lower_right - upper_right
    diff_four = diff_two - lower_left
    return (upper_left, lower_left, lower_right, diff_four, diff_one, diff_two, diff_three)


def reference(left_matrix, right_matrix):
    half_order = ORDER // 2
    lefts = left_terms(left_matrix[:half_order, :half_order], left_matrix[:half_order, half_order:],
                       left_matrix[half_order:, :half_order], left_matrix[half_order:, half_order:])
    rights = right_terms(right_matrix[:half_order, :half_order], right_matrix[:half_order, half_order:],
                         right_matrix[half_order:, :half_order], right_matrix[half_order:, half_order:])
    products = [multiply(lefts[index], rights[index]) for index in range(7)]
    partial_two = products[0] + products[5]
    partial_three = partial_two + products[6]
    partial_four = partial_two + products[4]
    upper_left = products[0] + products[1]
    upper_right = partial_four + products[2]
    lower_left = partial_three - products[3]
    lower_right = partial_three + products[4]
    return jnp.block([[upper_left, upper_right], [lower_left, lower_right]])
```

```python
import functools

import jax
import jax.numpy as jnp
from jax import lax
from jax.experimental import pallas as pl
from jax.experimental.pallas import tpu as pltpu
from jax.sharding import PartitionSpec as P

MESH = pl.DeviceIdType.MESH
CHUNKS = 4


def kernel(a_hbm, b_hbm, c_ref, a_buf, b_buf, relay, load_sem, a_sem, b_sem, relay_sem, send_sem):
    row, col = lax.axis_index("row"), lax.axis_index("col")
    y, x_hi = row // 2, row % 2
    x_lo, z, core = col // 8, (col // 2) % 4, col % 2
    x = x_hi * 2 + x_lo

    def device(x, y, z, core):
        return (y * 2 + x // 2, ((x % 2) * 4 + z) * 2 + core)

    z_up, z_down = device(x, y, (z + 1) % 4, core), device(x, y, (z + 3) % 4, core)
    y_up, y_down = device(x, (y + 1) % 4, z, core), device(x, (y + 3) % 4, z, core)
    x_pair = device(x_hi * 2 + 1 - x_lo, y, z, core)
    x_next = device(3 - x, y, z, core)
    twin = device(x, y, z, 1 - core)

    load_a = pltpu.make_async_copy(a_hbm, a_buf.at[0, 0], load_sem.at[0])
    load_b = pltpu.make_async_copy(b_hbm, b_buf.at[0], load_sem.at[1])
    load_a.start()
    load_b.start()

    barrier = pltpu.get_barrier_semaphore()
    for other in (z_up, z_down, y_up, y_down, x_pair, x_next, twin):
        pl.semaphore_signal(barrier, inc=1, device_id=other, device_id_type=MESH)
    c_ref[...] = jnp.zeros_like(c_ref)
    load_a.wait()
    load_b.wait()
    pl.semaphore_wait(barrier, 7)

    rows = a_buf.shape[2] // CHUNKS
    sent = []

    def send(src, dst, sem, to):
        copy = pltpu.make_async_remote_copy(
            src_ref=src,
            dst_ref=dst,
            send_sem=send_sem.at[len(sent)],
            recv_sem=sem,
            device_id=to,
            device_id_type=MESH,
        )
        copy.start()
        sent.append(copy)

    def part(q):
        return pl.ds(q * rows, rows)

    def a_send(src, q, slot, to):
        send(a_buf.at[0, src, part(q)], a_buf.at[0, slot, part(q)], a_sem.at[0, slot, q], to)

    def b_send(src, q, slot, to):
        send(b_buf.at[src, part(q)], b_buf.at[slot, part(q)], b_sem.at[slot, q], to)

    def a_twin(slot, q):
        send(a_buf.at[0, slot, part(q)], a_buf.at[1, slot, part(q)], a_sem.at[1, slot, q], twin)

    def a_wait(stream, slot, q):
        ref = a_buf.at[stream, slot, part(q)]
        pltpu.make_async_copy(ref, ref, a_sem.at[stream, slot, q]).wait()

    def b_wait(slot, q):
        ref = b_buf.at[slot, part(q)]
        pltpu.make_async_copy(ref, ref, b_sem.at[slot, q]).wait()

    def multiply(stage):
        @pl.loop(0, 8)
        def _(slot):
            d_x, d_z = slot // 4, slot % 4
            where = ((x_lo + d_x) % 2) * 4 + (z + d_z) % 4
            d_h, d_y = (where % 2 + x_hi) % 2, (where // 2 + 4 - y) % 4

            def stage_of(far, around):
                return jnp.where(far == 0, 1, jnp.where(around == 0, 2, jnp.where(around == 2, 4, 3)))

            ready = jnp.maximum(stage_of(d_x, d_z), stage_of(d_h, d_y))

            @pl.when(ready == stage)
            def _():
                for stream in range(2):
                    side = core if stream == 0 else 1 - core
                    b = b_buf[d_h * 4 + d_y, pl.ds(pl.multiple_of(side * 256, 256), 256)]
                    b_top = b.astype(jnp.bfloat16)
                    b_low = (b - b_top.astype(jnp.float32)).astype(jnp.bfloat16)
                    a = a_buf[stream, slot]
                    a_top = a.astype(jnp.bfloat16)
                    a_low = (a - a_top.astype(jnp.float32)).astype(jnp.bfloat16)
                    dot = functools.partial(jnp.dot, preferred_element_type=jnp.float32)
                    c_ref[...] += dot(a_top, b_top) + (dot(a_top, b_low) + dot(a_low, b_top))

    for q, p in zip((0, 1, 2, 3), (2, 3, 0, 1)):
        a_send(0, q, 3, z_up)
        a_send(0, p, 1, z_down)
        b_send(0, q, 3, y_up)
        b_send(0, p, 1, y_down)
        if q < 2:
            send(b_buf.at[0, part(q)], relay.at[0, q], relay_sem.at[0, q], x_pair)
            send(b_buf.at[0, part(q + 2)], relay.at[1, q], relay_sem.at[1, q], x_next)
    for q in range(3):
        a_send(0, q, 4, x_pair)
    for q in range(4):
        a_twin(0, q)

    for q in range(2):
        for which, to in ((0, x_next), (1, x_pair)):
            ref = relay.at[which, q]
            pltpu.make_async_copy(ref, ref, relay_sem.at[which, q]).wait()
            q_to = q + 2 * which
            send(ref, b_buf.at[4, part(q_to)], b_sem.at[4, q_to], to)
        a_wait(0, 3, q)
        a_send(3, q, 2, z_up)
        a_twin(3, q)
        a_wait(0, 1, q + 2)
        a_send(1, q + 2, 2, z_down)
        a_twin(1, q + 2)
        b_wait(3, q)
        b_send(3, q, 2, y_up)
        b_wait(1, q + 2)
        b_send(1, q + 2, 2, y_down)
    a_send(0, 3, 4, x_pair)

    for q in range(2):
        a_wait(0, 3, q + 2)
        a_twin(3, q + 2)
        a_wait(0, 1, q)
        a_twin(1, q)
        b_wait(3, q + 2)
        b_wait(1, q)
        a_wait(0, 4, q)
        a_send(4, q, 7, z_up)
        a_send(4, q, 5, z_down)
        a_twin(4, q)
        b_wait(4, q)
        b_send(4, q, 7, y_up)
        b_send(4, q, 5, y_down)
    for q in range(2, 4):
        a_wait(0, 4, q)
        a_send(4, q, 7, z_up)
        a_send(4, q, 5, z_down)
        a_twin(4, q)
        a_wait(0, 2, q - 2)
        a_twin(2, q - 2)
        a_wait(0, 2, q)
        a_twin(2, q)
        b_wait(2, q - 2)
        b_wait(2, q)
        b_wait(4, q)
        b_send(4, q, 7, y_up)
        b_send(4, q, 5, y_down)
    for slot in (0, 3, 1, 2):
        for q in range(4):
            a_wait(1, slot, q)
    multiply(1)
    for q in range(4):
        a_wait(1, 4, q)
    multiply(2)

    for q in range(4):
        a_wait(0, 7, q)
        if q < 2:
            a_send(7, q, 6, z_up)
        a_twin(7, q)
        a_wait(0, 5, q)
        if q >= 2:
            a_send(5, q, 6, z_down)
        a_twin(5, q)
        b_wait(7, q)
        if q < 2:
            b_send(7, q, 6, y_up)
        b_wait(5, q)
        if q >= 2:
            b_send(5, q, 6, y_down)
    for slot in (7, 5):
        for q in range(4):
            a_wait(1, slot, q)
    multiply(3)

    for q in (0, 2, 1, 3):
        a_wait(0, 6, q)
        a_twin(6, q)
        b_wait(6, q)
    for q in (0, 2, 1, 3):
        a_wait(1, 6, q)
    multiply(4)
    for copy in sent:
        copy.wait_send()


SENDS = 24 + 4 + 32 + 24 + 4 + 4


def body(left_matrix, right_matrix):
    rows, columns = left_matrix.shape
    part = rows // CHUNKS
    return pl.pallas_call(
        kernel,
        out_shape=jax.ShapeDtypeStruct((rows, columns), jnp.float32),
        in_specs=[pl.BlockSpec(memory_space=pl.ANY)] * 2,
        out_specs=pl.BlockSpec(memory_space=pltpu.VMEM),
        scratch_shapes=[
            pltpu.VMEM((2, 8, rows, columns), jnp.float32),
            pltpu.VMEM((8, rows, columns), jnp.float32),
            pltpu.VMEM((2, 2, part, columns), jnp.float32),
            pltpu.SemaphoreType.DMA((2,)),
            pltpu.SemaphoreType.DMA((2, 8, CHUNKS)),
            pltpu.SemaphoreType.DMA((8, CHUNKS)),
            pltpu.SemaphoreType.DMA((2, 2)),
            pltpu.SemaphoreType.DMA((SENDS,)),
        ],
        compiler_params=pltpu.CompilerParams(collective_id=0, has_side_effects=True),
    )(left_matrix, right_matrix)


def solution(mesh):
    placed = (P("row", "col"), P("row", "col"))
    return jax.shard_map(
        body, mesh=mesh, in_specs=placed, out_specs=P("row", "col"), check_vma=False
    )
```

```python
import functools

import jax
import jax.numpy as jnp
from jax import lax
from jax.experimental import pallas as pl
from jax.experimental.pallas import tpu as pltpu
from jax.sharding import PartitionSpec as P

MESH = pl.DeviceIdType.MESH
ROWS, COLUMNS = 512, 256
A_PARTS = {"U0": (0, 64), "U1": (64, 64), "D0": (128, 64), "D1": (192, 64), "X0": (256, 128), "X1": (384, 128)}
B_PARTS = {"U0": (0, 64), "U1": (64, 64), "D0": (128, 64), "D1": (192, 64), "U2": (256, 64), "D2": (320, 64), "X0": (384, 64), "X1": (448, 64)}
PAIR_FIRST = ("U0", "U1", "D0", "D1")
COPIES = 121
A_ORDER, B_ORDER = (0, 1, 6, 1, 2, 4, 8, 4), (0, 1, 3, 1, 3, 5, 7, 5)


def kernel(a_hbm, b_hbm, c_ref, a_buf, b_buf, relay, load_sem, recv_sem, send_sem):
    row, col = lax.axis_index("row"), lax.axis_index("col")
    y, x_hi = row // 2, row % 2
    x_lo, z, core = col // 8, (col // 2) % 4, col % 2
    x = x_hi * 2 + x_lo

    def device(x, y, z, core):
        return (y * 2 + x // 2, ((x % 2) * 4 + z) * 2 + core)

    z_up, z_down = device(x, y, (z + 1) % 4, core), device(x, y, (z + 3) % 4, core)
    y_up, y_down = device(x, (y + 1) % 4, z, core), device(x, (y + 3) % 4, z, core)
    x_pair = device(x_hi * 2 + 1 - x_lo, y, z, core)
    x_next = device(3 - x, y, z, core)
    twin = device(x, y, z, 1 - core)

    load_a = pltpu.make_async_copy(a_hbm, a_buf.at[0, 0], load_sem.at[0])
    load_b = pltpu.make_async_copy(b_hbm, b_buf.at[0], load_sem.at[1])
    load_a.start()
    load_b.start()

    barrier = pltpu.get_barrier_semaphore()
    for other in (z_up, z_down, y_up, y_down, x_pair, x_next, twin):
        pl.semaphore_signal(barrier, inc=1, device_id=other, device_id_type=MESH)
    c_ref[...] = jnp.zeros_like(c_ref)
    keys, partners = [], []
    for slot in range(8):
        where = ((x_lo + slot // 4) % 2) * 4 + (z + slot % 4) % 4
        d_h, d_y = (where % 2 + x_hi) % 2, (where // 2 + 4 - y) % 4
        partners.append(d_h * 4 + d_y)
        b_order = sum(jnp.where(partners[-1] == other, B_ORDER[other], 0) for other in range(8))
        keys.append(jnp.maximum(b_order, A_ORDER[slot]) * 8 + slot)
    places = [
        sum((keys[other] < keys[slot]).astype(jnp.int32) for other in range(8) if other != slot)
        for slot in range(8)
    ]

    def at_place(place, values):
        return sum(jnp.where(places[slot] == place, values[slot], 0) for slot in range(8))

    chosen = [(at_place(place, range(8)), at_place(place, partners)) for place in range(8)]

    load_a.wait()
    load_b.wait()
    pl.semaphore_wait(barrier, 7)

    sent, arrivals = [], {}

    def arrival(key):
        return recv_sem.at[arrivals.setdefault(key, len(arrivals))]

    def send(src, dst, key, to):
        copy = pltpu.make_async_remote_copy(
            src_ref=src,
            dst_ref=dst,
            send_sem=send_sem.at[len(sent)],
            recv_sem=arrival(key),
            device_id=to,
            device_id_type=MESH,
        )
        copy.start()
        sent.append(copy)

    def wait(ref, key):
        pltpu.make_async_copy(ref, ref, arrival(key)).wait()

    def part(table, first, last):
        return pl.ds(table[first][0], table[last][0] + table[last][1] - table[first][0])

    def a_part(slot, q):
        return a_buf.at[0, slot, part(A_PARTS, q, q)]

    def b_part(slot, q):
        return b_buf.at[slot, part(B_PARTS, q, q)]

    def relay_part(slot, q):
        return relay.at[slot // 2, part(B_PARTS, q, q)]

    def a_send(src, q, slot, to):
        send(a_part(src, q), a_part(slot, q), ("a", slot, q), to)

    def a_wait(slot, q):
        wait(a_part(slot, q), ("a", slot, q))

    def b_send(src, q, slot, to):
        send(b_part(src, q), b_part(slot, q), ("b", slot, q), to)

    def b_wait(slot, q):
        wait(b_part(slot, q), ("b", slot, q))

    def leg_one(slot, q):
        send(b_part(slot, q), relay_part(slot, q), ("r", slot, q), x_pair if pair_first(slot, q) else x_next)

    def relay_wait(slot, q):
        wait(relay_part(slot, q), ("r", slot, q))

    def leg_two(slot, q):
        send(relay_part(slot, q), b_part(4 + slot, q), ("b", 4 + slot, q), x_next if pair_first(slot, q) else x_pair)

    def pair_first(slot, q):
        return q in PAIR_FIRST if slot == 0 else q == "X0"

    def twin_send(slot, first, last):
        at = part(A_PARTS, first, last)
        send(a_buf.at[0, slot, at], a_buf.at[1, slot, at], ("t", slot, first), twin)

    def twin_wait(slot, first, last):
        wait(a_buf.at[1, slot, part(A_PARTS, first, last)], ("t", slot, first))

    def product(place):
        slot, other = chosen[place]
        total = None
        for stream in range(2):
            side = core if stream == 0 else 1 - core
            b = b_buf[other, pl.ds(pl.multiple_of(side * 256, 256), 256)]
            b_top = b.astype(jnp.bfloat16)
            b_low = (b - b_top.astype(jnp.float32)).astype(jnp.bfloat16)
            a = a_buf[stream, slot]
            a_top = a.astype(jnp.bfloat16)
            a_low = (a - a_top.astype(jnp.float32)).astype(jnp.bfloat16)
            dot = functools.partial(jnp.dot, preferred_element_type=jnp.float32)
            part = dot(a_top, b_top) + (dot(a_top, b_low) + dot(a_low, b_top))
            total = part if total is None else total + part
        c_ref[...] += total

    a_send(0, "X0", 3, z_up)
    a_send(0, "U0", 3, z_up)
    a_send(0, "U1", 3, z_up)
    a_send(0, "D0", 3, z_up)
    a_send(0, "D1", 3, z_up)
    a_send(0, "X1", 3, z_up)
    a_send(0, "X1", 1, z_down)
    a_send(0, "D0", 1, z_down)
    a_send(0, "D1", 1, z_down)
    a_send(0, "U0", 1, z_down)
    a_send(0, "U1", 1, z_down)
    a_send(0, "X0", 1, z_down)
    b_send(0, "X0", 3, y_up)
    b_send(0, "U0", 3, y_up)
    b_send(0, "U1", 3, y_up)
    b_send(0, "U2", 3, y_up)
    b_send(0, "D0", 3, y_up)
    b_send(0, "D1", 3, y_up)
    b_send(0, "D2", 3, y_up)
    b_send(0, "X1", 3, y_up)
    b_send(0, "X1", 1, y_down)
    b_send(0, "D0", 1, y_down)
    b_send(0, "D1", 1, y_down)
    b_send(0, "D2", 1, y_down)
    b_send(0, "U0", 1, y_down)
    b_send(0, "U1", 1, y_down)
    b_send(0, "U2", 1, y_down)
    b_send(0, "X0", 1, y_down)
    leg_one(0, "U2")
    leg_one(0, "D2")
    leg_one(0, "X0")
    leg_one(0, "X1")
    leg_one(0, "U0")
    leg_one(0, "D0")
    leg_one(0, "U1")
    leg_one(0, "D1")
    a_send(0, "U0", 4, x_pair)
    a_send(0, "D0", 4, x_pair)
    a_send(0, "U1", 4, x_pair)
    a_send(0, "D1", 4, x_pair)
    twin_send(0, "U0", "X1")
    b_wait(3, "X0")
    b_send(3, "X0", 2, y_up)
    b_wait(1, "X1")
    b_send(1, "X1", 2, y_down)
    relay_wait(0, "U2")
    leg_two(0, "U2")
    a_send(0, "X0", 4, x_pair)
    a_send(0, "X1", 4, x_pair)
    relay_wait(0, "U0")
    leg_two(0, "U0")
    a_wait(3, "X0")
    a_send(3, "X0", 2, z_up)
    a_wait(1, "X1")
    a_send(1, "X1", 2, z_down)
    relay_wait(0, "D2")
    leg_two(0, "D2")
    relay_wait(0, "D0")
    leg_two(0, "D0")
    relay_wait(0, "X0")
    leg_two(0, "X0")
    relay_wait(0, "U1")
    leg_two(0, "U1")
    relay_wait(0, "X1")
    leg_two(0, "X1")
    relay_wait(0, "D1")
    leg_two(0, "D1")
    b_wait(4, "U0")
    b_send(4, "U0", 7, y_up)
    a_wait(4, "U0")
    a_send(4, "U0", 7, z_up)
    b_wait(4, "D0")
    b_send(4, "D0", 7, y_up)
    b_send(4, "D0", 5, y_down)
    b_send(4, "U0", 5, y_down)
    a_wait(4, "D0")
    a_send(4, "D0", 7, z_up)
    a_send(4, "D0", 5, z_down)
    a_send(4, "U0", 5, z_down)
    b_wait(4, "U1")
    b_send(4, "U1", 7, y_up)
    a_wait(4, "U1")
    a_send(4, "U1", 7, z_up)
    a_wait(1, "D0")
    a_wait(1, "D1")
    a_wait(1, "U0")
    a_wait(1, "U1")
    a_wait(1, "X0")
    twin_send(1, "U0", "X1")
    a_wait(3, "U0")
    a_wait(3, "U1")
    a_wait(3, "D0")
    a_wait(3, "D1")
    a_wait(3, "X1")
    twin_send(3, "U0", "X1")
    b_wait(4, "D1")
    b_send(4, "D1", 7, y_up)
    b_wait(3, "U0")
    b_send(3, "U0", 2, y_up)
    b_wait(3, "U1")
    b_send(3, "U1", 2, y_up)
    b_wait(3, "U2")
    b_send(3, "U2", 2, y_up)
    b_send(4, "D1", 5, y_down)
    b_send(4, "U1", 5, y_down)
    b_wait(1, "D0")
    b_send(1, "D0", 2, y_down)
    b_wait(1, "D1")
    b_send(1, "D1", 2, y_down)
    b_wait(1, "D2")
    b_send(1, "D2", 2, y_down)
    a_wait(4, "D1")
    a_send(4, "D1", 7, z_up)
    a_send(4, "D1", 5, z_down)
    a_send(4, "U1", 5, z_down)
    b_wait(2, "X0")
    leg_one(2, "X0")
    b_wait(2, "X1")
    leg_one(2, "X1")
    b_wait(4, "U2")
    b_send(4, "U2", 7, y_up)
    b_send(4, "U2", 5, y_down)
    a_wait(4, "X0")
    a_send(4, "X0", 7, z_up)
    a_send(4, "X0", 5, z_down)
    relay_wait(2, "X1")
    leg_two(2, "X1")
    a_wait(2, "X0")
    a_send(2, "X0", 6, x_pair)
    a_wait(2, "X1")
    a_send(2, "X1", 6, x_pair)
    a_wait(4, "X1")
    a_send(4, "X1", 7, z_up)
    a_send(3, "U0", 2, z_up)
    a_send(3, "U1", 2, z_up)
    a_wait(7, "U0")
    a_send(7, "U0", 6, z_up)
    a_wait(7, "U1")
    a_send(7, "U1", 6, z_up)
    a_send(4, "X1", 5, z_down)
    a_send(1, "D0", 2, z_down)
    a_send(1, "D1", 2, z_down)
    a_wait(5, "D0")
    a_send(5, "D0", 6, z_down)
    a_wait(5, "D1")
    a_send(5, "D1", 6, z_down)
    twin_send(4, "U0", "X1")
    a_wait(7, "D0")
    a_wait(7, "D1")
    twin_send(7, "U0", "D1")
    a_wait(5, "U0")
    a_wait(5, "U1")
    twin_send(5, "U0", "D1")
    b_wait(4, "D2")
    b_send(4, "D2", 7, y_up)
    b_send(4, "D2", 5, y_down)
    twin_wait(0, "U0", "X1")
    b_wait(3, "D0")
    b_wait(1, "U0")
    b_wait(3, "D1")
    b_wait(1, "U1")
    b_wait(3, "D2")
    b_wait(1, "U2")
    b_wait(3, "X1")
    b_wait(1, "X0")
    twin_wait(1, "U0", "X1")
    twin_wait(3, "U0", "X1")
    twin_wait(4, "U0", "X1")
    product(0)
    b_wait(4, "X0")
    b_send(4, "X0", 7, y_up)
    b_send(4, "X0", 5, y_down)
    b_wait(4, "X1")
    b_send(4, "X1", 7, y_up)
    b_wait(7, "U0")
    b_send(7, "U0", 6, y_up)
    b_wait(7, "U1")
    b_send(7, "U1", 6, y_up)
    b_send(4, "X1", 5, y_down)
    b_wait(5, "D0")
    b_send(5, "D0", 6, y_down)
    b_wait(5, "D1")
    b_send(5, "D1", 6, y_down)
    b_wait(2, "U0")
    b_wait(2, "D0")
    b_wait(2, "U1")
    b_wait(2, "D1")
    b_wait(2, "U2")
    b_wait(2, "D2")
    product(1)
    b_wait(7, "U2")
    b_send(7, "U2", 6, y_up)
    relay_wait(2, "X0")
    leg_two(2, "X0")
    a_wait(7, "X0")
    a_wait(7, "X1")
    twin_send(7, "X0", "X1")
    a_wait(5, "X0")
    a_wait(5, "X1")
    twin_send(5, "X0", "X1")
    b_wait(5, "D2")
    b_send(5, "D2", 6, y_down)
    twin_wait(7, "U0", "D1")
    twin_wait(5, "U0", "D1")
    twin_wait(7, "X0", "X1")
    twin_wait(5, "X0", "X1")
    product(2)
    a_wait(2, "U0")
    a_wait(2, "D0")
    a_wait(2, "U1")
    a_wait(2, "D1")
    twin_send(2, "U0", "X1")
    a_wait(6, "X0")
    twin_send(6, "X0", "X0")
    b_wait(7, "D0")
    b_wait(5, "U0")
    b_wait(7, "D1")
    b_wait(5, "U1")
    b_wait(5, "U2")
    b_wait(7, "D2")
    b_wait(7, "X0")
    b_wait(5, "X0")
    b_wait(7, "X1")
    b_wait(5, "X1")
    product(3)
    product(4)
    twin_wait(2, "U0", "X1")
    product(5)
    a_wait(6, "U0")
    a_wait(6, "U1")
    twin_send(6, "U0", "U1")
    a_wait(6, "D0")
    a_wait(6, "D1")
    twin_send(6, "D0", "D1")
    a_wait(6, "X1")
    twin_send(6, "X1", "X1")
    b_wait(6, "X1")
    b_wait(6, "X0")
    b_wait(6, "U0")
    b_wait(6, "D0")
    b_wait(6, "U1")
    b_wait(6, "D1")
    b_wait(6, "U2")
    b_wait(6, "D2")
    product(6)
    twin_wait(6, "X0", "X0")
    twin_wait(6, "U0", "U1")
    twin_wait(6, "D0", "D1")
    twin_wait(6, "X1", "X1")
    product(7)
    for copy in sent:
        copy.wait_send()


def body(left_matrix, right_matrix):
    kept = functools.partial(pltpu.with_memory_space_constraint, memory_space=pltpu.HBM)
    return pl.pallas_call(
        kernel,
        out_shape=jax.ShapeDtypeStruct((ROWS, COLUMNS), jnp.float32),
        in_specs=[pl.BlockSpec(memory_space=pl.ANY)] * 2,
        out_specs=pl.BlockSpec(memory_space=pltpu.VMEM),
        scratch_shapes=[
            pltpu.VMEM((2, 8, ROWS, COLUMNS), jnp.float32),
            pltpu.VMEM((8, ROWS, COLUMNS), jnp.float32),
            pltpu.VMEM((2, ROWS, COLUMNS), jnp.float32),
            pltpu.SemaphoreType.DMA((2,)),
            pltpu.SemaphoreType.DMA((COPIES,)),
            pltpu.SemaphoreType.DMA((COPIES,)),
        ],
        compiler_params=pltpu.CompilerParams(
            collective_id=0, has_side_effects=True, vmem_limit_bytes=24 * 2**20
        ),
    )(kept(left_matrix), kept(right_matrix))


def solution(mesh):
    placed = (P("row", "col"), P("row", "col"))
    return jax.shard_map(
        body, mesh=mesh, in_specs=placed, out_specs=P("row", "col"), check_vma=False
    )
```
